8 devices in a mesh: dp: 1 (over z), sp: 8 (over y, x, core).
Axes of the slice: x: 2, y: 2, z: 1, core: 2. Of those that a mesh axis runs over, the one named last changes fastest.
Arguments:
- x: bfloat16 [8, 4096], P('dp')
- lens: int32 [8], P('dp')
- wq: bfloat16 [2, 4096, 4096], replicated
- wk: bfloat16 [2, 4096, 1024], replicated
- wv: bfloat16 [2, 4096, 1024], replicated
- wo: bfloat16 [2, 4096, 4096], P(None, 'sp')
- w1: bfloat16 [2, 4096, 16384], P(None, None, 'sp')
- w2: bfloat16 [2, 16384, 4096], P(None, 'sp')
- g1: bfloat16 [2, 4096], replicated
- g2: bfloat16 [2, 4096], replicated
- kc: bfloat16 [2, 8, 4096, 8, 128], P(None, 'dp', 'sp')
- vc: bfloat16 [2, 8, 4096, 8, 128], P(None, 'dp', 'sp')
Outputs:
- output 1: bfloat16 [8, 4096], P('dp')
- output 2: bfloat16 [2, 8, 4096, 8, 128], P(None, 'dp', 'sp')
- output 3: bfloat16 [2, 8, 4096, 8, 128], P(None, 'dp', 'sp')
All inputs are finite; a program needn't handle non-finite values.
Results may differ from the reference program's by a relative error of at most 0.00860115.
Values are sent between devices in bfloat16 or wider.
A program may use at most 1 GiB of HBM per device.

```python
import math
import jax
import jax.numpy as jnp
from jax import lax

B = 8
S_DEV = 512
SEQ = 8
D = 4096
HEADS = 32
KV_HEADS = 8
HEAD = 128
LAYERS = 2
S = S_DEV * SEQ
G = HEADS // KV_HEADS
FF = 4 * D
BLOCK = min(S_DEV, 1024)
EPS = 1e-6


def _rms(h, g):
    r = lax.rsqrt(jnp.mean(h * h, axis=-1, keepdims=True) + EPS)
    return (h * r * g.astype(jnp.float32)).astype(jnp.bfloat16)


def _mm(a, w):
    return jnp.dot(a, w, preferred_element_type=jnp.float32)


def _cache(key, t):
    k = jax.random.split(key, 7)
    ph = jax.random.uniform(k[0], (B, 3), jnp.float32)
    fr = jax.random.uniform(k[1], (B, 3), jnp.float32, 1.0, 3.0)
    wave = jnp.sin(2.0 * math.pi * (fr[:, None, :] * t[None, :, None] + ph[:, None, :]))
    kdir = jax.random.normal(k[2], (B, 1, KV_HEADS, HEAD), jnp.float32)
    u1 = jax.random.normal(k[3], (B, 1, KV_HEADS, HEAD), jnp.float32)
    u2 = jax.random.normal(k[4], (B, 1, KV_HEADS, HEAD), jnp.float32)
    kc = jax.random.normal(k[5], (B, S, KV_HEADS, HEAD), jnp.float32) + wave[:, :, 0, None, None] * kdir
    vc = (0.5 * jax.random.normal(k[6], (B, S, KV_HEADS, HEAD), jnp.float32)
          + wave[:, :, 1, None, None] * u1 + wave[:, :, 2, None, None] * u2)
    return kc.astype(jnp.bfloat16), vc.astype(jnp.bfloat16)


def _lengths(key):
    draws = jax.random.randint(key, (B,), 0, 256, dtype=jnp.int32)
    scaled = draws * (S - 1) // 255
    lens = scaled * draws // 255 + 1
    return lens.at[0].set(S).astype(jnp.int32)


def setup_inputs(seed: int = 0, part: int = 0) -> dict:
    key = jax.random.key(seed)
    ks = jax.random.split(key, 8)
    kp = jax.random.split(jax.random.fold_in(key, part), 3)
    gamma = (math.log(S) - 1.0) / math.sqrt(HEAD)
    wk = jax.random.normal(ks[0], (LAYERS, D, KV_HEADS, 1, HEAD), jnp.float32) * D ** -0.5
    wq = gamma * wk + jax.random.normal(ks[1], (LAYERS, D, KV_HEADS, G, HEAD), jnp.float32) * D ** -0.5
    wv = jax.random.normal(ks[2], (LAYERS, D, KV_HEADS * HEAD), jnp.float32) * D ** -0.5
    wo = jax.random.normal(ks[3], (LAYERS, HEADS * HEAD, D), jnp.float32) * (HEADS * HEAD) ** -0.5
    w1 = jax.random.normal(ks[4], (LAYERS, D, FF), jnp.float32) * D ** -0.5
    w2 = jax.random.normal(ks[5], (LAYERS, FF, D), jnp.float32) * FF ** -0.5
    g1 = 1.0 + 0.1 * jax.random.normal(ks[6], (LAYERS, D), jnp.float32)
    g2 = 1.0 + 0.1 * jax.random.normal(ks[7], (LAYERS, D), jnp.float32)
    t = jnp.arange(S, dtype=jnp.float32) / S
    ck = jax.random.split(kp[2], LAYERS)
    caches = [_cache(ck[i], t) for i in range(LAYERS)]
    bf = jnp.bfloat16
    return {
        'x': jax.random.normal(kp[0], (B, D), jnp.float32).astype(bf),
        'lens': _lengths(kp[1]),
        'wq': wq.reshape(LAYERS, D, HEADS * HEAD).astype(bf),
        'wk': wk.reshape(LAYERS, D, KV_HEADS * HEAD).astype(bf),
        'wv': wv.astype(bf),
        'wo': wo.astype(bf),
        'w1': w1.astype(bf),
        'w2': w2.astype(bf),
        'g1': g1.astype(bf),
        'g2': g2.astype(bf),
        'kc': jnp.stack([c[0] for c in caches]),
        'vc': jnp.stack([c[1] for c in caches]),
    }


def _attend(q, kc, vc, lens):
    qf = q.astype(jnp.float32)

    def body(carry, i):
        m, l, o = carry
        k = lax.dynamic_slice_in_dim(kc, i * BLOCK, BLOCK, axis=1).astype(jnp.float32)
        v = lax.dynamic_slice_in_dim(vc, i * BLOCK, BLOCK, axis=1).astype(jnp.float32)
        s = jnp.einsum('bkgd,bskd->bkgs', qf, k) * HEAD ** -0.5
        posn = i * BLOCK + jnp.arange(BLOCK)
        s = jnp.where((posn[None, :] < lens[:, None])[:, None, None, :], s, -jnp.inf)
        mn = jnp.maximum(m, jnp.max(s, axis=-1))
        c = jnp.exp(m - mn)
        p = jnp.exp(s - mn[..., None])
        o = o * c[..., None] + jnp.einsum('bkgs,bskd->bkgd', p, v)
        return (mn, l * c + jnp.sum(p, axis=-1), o), None

    init = (jnp.full((B, KV_HEADS, G), -jnp.inf, jnp.float32),
            jnp.zeros((B, KV_HEADS, G), jnp.float32),
            jnp.zeros((B, KV_HEADS, G, HEAD), jnp.float32))
    (m, l, o), _ = lax.scan(body, init, jnp.arange(S // BLOCK))
    return o / l[..., None]


def reference(x, lens, wq, wk, wv, wo, w1, w2, g1, g2, kc, vc):
    posn = jnp.arange(S)
    write = (posn[None, :] == (lens - 1)[:, None])[:, :, None, None]

    def layer(h, w):
        wq_, wk_, wv_, wo_, w1_, w2_, g1_, g2_, kc_, vc_ = w
        xn = _rms(h, g1_)
        q = _mm(xn, wq_).astype(jnp.bfloat16).reshape(B, KV_HEADS, G, HEAD)
        k = _mm(xn, wk_).astype(jnp.bfloat16).reshape(B, 1, KV_HEADS, HEAD)
        v = _mm(xn, wv_).astype(jnp.bfloat16).reshape(B, 1, KV_HEADS, HEAD)
        kn = jnp.where(write, k, kc_)
        vn = jnp.where(write, v, vc_)
        o = _attend(q, kn, vn, lens).astype(jnp.bfloat16).reshape(B, HEADS * HEAD)
        h = h + _mm(o, wo_)
        u = jax.nn.gelu(_mm(_rms(h, g2_), w1_)).astype(jnp.bfloat16)
        h = h + _mm(u, w2_)
        return h, (kn, vn)

    h, (kn, vn) = lax.scan(layer, x.astype(jnp.float32), (wq, wk, wv, wo, w1, w2, g1, g2, kc, vc))
    return h.astype(jnp.bfloat16), kn, vn
```

```python
import functools

import jax
import jax.numpy as jnp
from jax import lax
from jax.experimental import pallas as pl
from jax.experimental.pallas import tpu as pltpu
from jax.sharding import PartitionSpec as P

EPS = 1e-6
N = 8
B = 8
D = 4096
KVH = 8
G = 4
DH = 128
SD = 512
R = SD * KVH
C = D // N
QW = (G + 2) * DH
FD = 2048
FC = 512
NF = FD // FC
SCALE = DH ** -0.5
F32, BF16 = jnp.float32, jnp.bfloat16
MESH = pl.DeviceIdType.MESH
VM = pl.BlockSpec(memory_space=pltpu.VMEM)
HBM = pl.BlockSpec(memory_space=pltpu.HBM)
SM = pl.BlockSpec(memory_space=pltpu.SMEM)
LIMIT = 67_043_328
DMA = pltpu.SemaphoreType.DMA
SDS = jax.ShapeDtypeStruct


def _peer(me, m):
    return ((me // 4 + m // 4) % 2) * 4 + ((me // 2 + m // 2) % 2) * 2 + (me + m) % 2


def _remote(src, dst, ssem, rsem, dev):
    return pltpu.make_async_remote_copy(src_ref=src, dst_ref=dst, send_sem=ssem, recv_sem=rsem,
                                        device_id={'sp': dev}, device_id_type=MESH)


def _barrier(me):
    bar = pltpu.get_barrier_semaphore()
    for m in range(1, N):
        pl.semaphore_signal(bar, inc=1, device_id={'sp': _peer(me, m)}, device_id_type=MESH)
    pl.semaphore_wait(bar, N - 1)


def _dot(a, w):
    return jnp.dot(a, w, preferred_element_type=F32)


def _qkv_copies(l, me, wq, wk, wv, wqb, wkvb, sem):
    cols = pl.ds(pl.multiple_of(me * G * DH, G * DH), G * DH)
    one = pl.ds(pl.multiple_of(me * DH, DH), DH)
    return (pltpu.make_async_copy(wq.at[l, :, cols], wqb, sem.at[0]),
            pltpu.make_async_copy(wk.at[l, :, one], wkvb.at[0], sem.at[1]),
            pltpu.make_async_copy(wv.at[l, :, one], wkvb.at[1], sem.at[2]))


def _qkv(xn, wqb, wkvb, cps, out):
    cps[0].wait()
    out[:, :G * DH] = _dot(xn, wqb[...]).astype(BF16)
    cps[1].wait()
    cps[2].wait()
    out[:, G * DH:(G + 1) * DH] = _dot(xn, wkvb[0]).astype(BF16)
    out[:, (G + 1) * DH:] = _dot(xn, wkvb[1]).astype(BF16)


def _bcast_start(me, buf, ssem, rsem):
    def body(t, _):
        _remote(buf.at[me], buf.at[me], ssem.at[t], rsem.at[me], _peer(me, 7 - t)).start()
        return 0
    lax.fori_loop(0, N - 1, body, 0)


def _bcast_wait(me, buf, ssem, rsem):
    def body(t, _):
        s = _peer(me, 1 + t)
        _remote(buf.at[me], buf.at[s], ssem.at[t], rsem.at[s], s).wait_recv()
        return 0
    lax.fori_loop(0, N - 1, body, 0)

    def done(t, _):
        _remote(buf.at[me], buf.at[me], ssem.at[t], rsem.at[me], _peer(me, 7 - t)).wait_send()
        return 0
    lax.fori_loop(0, N - 1, done, 0)


def _split_heads(qkv, qf):
    for j in range(G + 2):
        qf[j] = qkv[:, :, j * DH:(j + 1) * DH].astype(F32).reshape(N * B, DH)


def _attend(b, lim, qf, kb, vb, o_out, ml_out):
    q = jnp.concatenate([qf[g, pl.ds(b, KVH, stride=B), :] for g in range(G)], axis=0).astype(BF16)
    s = lax.dot_general(q, kb, (((1,), (1,)), ((), ())), preferred_element_type=F32) * SCALE
    col = lax.broadcasted_iota(jnp.int32, s.shape, 1)
    row = lax.broadcasted_iota(jnp.int32, s.shape, 0)
    s = jnp.where(((col & 7) == (row & 7)) & (col < lim * KVH), s, -jnp.inf)
    m = jnp.max(s, axis=-1, keepdims=True)
    p = jnp.exp(s - jnp.where(m == -jnp.inf, 0.0, m))
    den = jnp.sum(p, axis=-1, keepdims=True)
    o = _dot(p.astype(BF16), vb)
    lane = lax.broadcasted_iota(jnp.int32, (KVH, DH), 1)
    ml = jnp.zeros((KVH, DH), F32)
    for g in range(G):
        rows = slice(g * KVH, (g + 1) * KVH)
        o_out[pl.ds(g * B + b, KVH, stride=G * B), :] = o[rows]
        ml = jnp.where(lane == g, m[rows], ml)
        ml = jnp.where(lane == G + g, den[rows], ml)
    ml_out[pl.ds(b, KVH, stride=B), :] = ml


def _new_rows(b, qf, k_out, v_out):
    k_out[b] = qf[G, pl.ds(b, KVH, stride=B), :].astype(BF16)
    v_out[b] = qf[G + 1, pl.ds(b, KVH, stride=B), :].astype(BF16)


def _k1(x, g1, wq, wk, wv, qkv, xn, wqb, wkvb, wsem, ssem, rsem):
    me = lax.axis_index('sp')
    cps = _qkv_copies(0, me, wq, wk, wv, wqb, wkvb, wsem)
    for c in cps:
        c.start()
    h = x[...].astype(F32)
    r = lax.rsqrt(jnp.mean(h * h, axis=-1, keepdims=True) + EPS)
    xn[...] = (h * r * g1[0:1, :].astype(F32)).astype(BF16)
    _barrier(me)
    _qkv(xn[...], wqb, wkvb, cps, qkv.at[me])
    _bcast_start(me, qkv, ssem, rsem)
    _bcast_wait(me, qkv, ssem, rsem)


def _k2(lens, qkv, kc, vc, kn, vn, o, ml, k0, v0, qf, kb, vb, rsem, wsem):
    me = lax.axis_index('sp')

    def copies(l, b):
        return ((pltpu.make_async_copy(kc.at[l, b], kb.at[l, b], rsem.at[0, l, b]),
                 pltpu.make_async_copy(vc.at[l, b], vb.at[l, b], rsem.at[1, l, b])),
                (pltpu.make_async_copy(kb.at[l, b], kn.at[l, b], wsem.at[0, l, b]),
                 pltpu.make_async_copy(vb.at[l, b], vn.at[l, b], wsem.at[1, l, b])))

    for l in range(2):
        for b in range(B):
            for c in copies(l, b)[0]:
                c.start()
    _split_heads(qkv, qf)

    def turn(l, b):
        rd, wr = copies(l, b)
        for c in rd:
            c.wait()
        for c in wr:
            c.start()

    def body(b, _):
        turn(0, b)
        _new_rows(b, qf, k0, v0)
        _attend(b, lens[b] - 1 - me * SD, qf, kb[0, b], vb[0, b], o, ml)
        return 0
    lax.fori_loop(0, B, body, 0)

    def rest(b, _):
        turn(1, b)
        return 0
    lax.fori_loop(0, B, rest, 0)

    def drain(b, _):
        for l in range(2):
            for c in copies(l, b)[1]:
                c.wait()
        return 0
    lax.fori_loop(0, B, drain, 0)


def _main(x, lens, g1, g2, qkv0, o0, ml0, wq, wk, wv, wo, w1, w2, kc, vc, y, k1, v1,
          wqb, wkvb, wob, w1b, w2b, kb, vb, xn, u, qkv1, qf, o1, orecv, mlrecv, rs_send, rs_recv, ag, yg, ml1,
          qsem, osem, w1sem, w2sem, ksem, vsem, a_s, a_r, m_s, m_r, rs_s, rs_r, ag_s, ag_r, q_s, q_r, y_s, y_r):
    me = lax.axis_index('sp')
    mine = pl.ds(pl.multiple_of(me * C, C), C)

    def wo_copy(l, t):
        cols = pl.ds(pl.multiple_of(_peer(me, 7 - t) * C, C), C)
        return pltpu.make_async_copy(wo.at[l, :, cols], wob.at[t], osem.at[t])

    def w1_copy(l, t):
        return pltpu.make_async_copy(w1.at[l, :, pl.ds(pl.multiple_of(t * FC, FC), FC)], w1b.at[t], w1sem.at[t])

    def w2_copy(l, t):
        cols = pl.ds(pl.multiple_of(_peer(me, 7 - t) * C, C), C)
        return pltpu.make_async_copy(w2.at[l, :, cols], w2b.at[t], w2sem.at[t])

    def kv_copies(b):
        return (pltpu.make_async_copy(kc.at[1, b], kb.at[b], ksem.at[b]),
                pltpu.make_async_copy(vc.at[1, b], vb.at[b], vsem.at[b]))

    for t in range(N):
        wo_copy(0, t).start()
    for t in range(NF):
        w1_copy(0, t).start()
    for t in range(N):
        w2_copy(0, t).start()
    qcps = _qkv_copies(1, me, wq, wk, wv, wqb, wkvb, qsem)
    for c in qcps:
        c.start()
    for b in range(B):
        for c in kv_copies(b):
            c.start()
    _barrier(me)

    def exchange(l, o, ml):
        def cps(t):
            d = _peer(me, 7 - t)
            return (_remote(o.at[pl.ds(pl.multiple_of(d * 32, 32), 32)], orecv.at[l, me], a_s.at[l, t], a_r.at[l, me], d),
                    _remote(ml.at[pl.ds(pl.multiple_of(d * 8, 8), 8)], mlrecv.at[l, me], m_s.at[l, t], m_r.at[l, me], d))

        def start(t, _):
            for c in cps(t):
                c.start()
            return 0
        lax.fori_loop(0, N - 1, start, 0)
        orecv[l, me] = o[pl.ds(pl.multiple_of(me * 32, 32), 32)]
        mlrecv[l, me] = ml[pl.ds(pl.multiple_of(me * 8, 8), 8)]

        def wait(t, _):
            s = _peer(me, 1 + t)
            _remote(o.at[pl.ds(0, 32)], orecv.at[l, s], a_s.at[l, t], a_r.at[l, s], s).wait_recv()
            _remote(ml.at[pl.ds(0, 8)], mlrecv.at[l, s], m_s.at[l, t], m_r.at[l, s], s).wait_recv()
            return 0
        lax.fori_loop(0, N - 1, wait, 0)

        def sent(t, _):
            for c in cps(t):
                c.wait_send()
            return 0
        lax.fori_loop(0, N - 1, sent, 0)

    def combine(l, own):
        k = own[:, G * DH:(G + 1) * DH]
        v = own[:, (G + 1) * DH:]
        out = []
        for g in range(G):
            sn = jnp.sum(own[:, g * DH:(g + 1) * DH] * k, axis=-1, keepdims=True) * SCALE
            ms = [mlrecv[l, s, :, g:g + 1] for s in range(N)]
            mt = functools.reduce(jnp.maximum, ms, sn)
            w = jnp.exp(sn - mt)
            den, num = w, w * v
            for s in range(N):
                w = jnp.exp(ms[s] - mt)
                den = den + w * mlrecv[l, s, :, G + g:G + g + 1]
                num = num + w * orecv[l, s, g * B:(g + 1) * B, :]
            out.append((num / den).astype(BF16))
        return jnp.concatenate(out, axis=-1)

    def reduce_scatter(use, a, wb, wait, again):
        def copy(t):
            return _remote(rs_send.at[use, t], rs_recv.at[use, me], rs_s.at[use, t], rs_r.at[use, me], _peer(me, 7 - t))

        def step(t, _):
            wait(t)
            rs_send[use, t] = _dot(a[...], wb[t])

            @pl.when(t < N - 1)
            def _():
                copy(t).start()
            if again is not None:
                again(t)
            return 0
        lax.fori_loop(0, N, step, 0)

        def add(t, acc):
            s = _peer(me, 1 + t)
            _remote(rs_send.at[use, t], rs_recv.at[use, s], rs_s.at[use, t], rs_r.at[use, s], s).wait_recv()
            return acc + rs_recv[use, s]
        acc = lax.fori_loop(0, N - 1, add, rs_send[use, N - 1])

        def sent(t, _):
            copy(t).wait_send()
            return 0
        lax.fori_loop(0, N - 1, sent, 0)
        return acc

    def gather_norm(use, hs, g):
        ag[use, me] = hs
        _bcast_start(me, ag.at[use], ag_s.at[use], ag_r.at[use])
        _bcast_wait(me, ag.at[use], ag_s.at[use], ag_r.at[use])
        ss = jnp.zeros((B, C), F32)
        for c in range(N):
            ss = ss + ag[use, c] * ag[use, c]
        r = lax.rsqrt(jnp.sum(ss, axis=-1, keepdims=True) / D + EPS)
        for c in range(N):
            xn[:, c * C:(c + 1) * C] = (ag[use, c] * r * g[:, c * C:(c + 1) * C].astype(F32)).astype(BF16)

    def layer(l, own, hs):
        first = l == 0
        u[:, :C] = combine(l, own)
        hs = hs + reduce_scatter(2 * l, u.at[:, :C], wob, lambda t: wo_copy(l, t).wait(),
                                 (lambda t: wo_copy(1, t).start()) if first else None)
        gather_norm(2 * l, hs, g2[l:l + 1, :])

        def up(t, _):
            w1_copy(l, t).wait()
            z = _dot(xn[...], w1b[t])
            u[:, pl.ds(pl.multiple_of(t * FC, FC), FC)] = jax.nn.gelu(z).astype(BF16)
            if first:
                w1_copy(1, t).start()
            return 0
        lax.fori_loop(0, NF, up, 0)
        return hs + reduce_scatter(2 * l + 1, u, w2b, lambda t: w2_copy(l, t).wait(),
                                   (lambda t: w2_copy(1, t).start()) if first else None)

    exchange(0, o0, ml0)
    hs = layer(0, qkv0[me].astype(F32), x[:, mine].astype(F32))
    gather_norm(1, hs, g1[1:2, :])
    _qkv(xn[...], wqb, wkvb, qcps, qkv1.at[me])
    _bcast_start(me, qkv1, q_s, q_r)
    _bcast_wait(me, qkv1, q_s, q_r)
    _split_heads(qkv1, qf)

    def att(b, _):
        for c in kv_copies(b):
            c.wait()
        _new_rows(b, qf, k1, v1)
        _attend(b, lens[b] - 1 - me * SD, qf, kb[b], vb[b], o1, ml1)
        return 0
    lax.fori_loop(0, B, att, 0)
    exchange(1, o1, ml1)
    hs = layer(1, qkv1[me].astype(F32), hs)
    yg[me] = hs.astype(BF16)
    _bcast_start(me, yg, y_s, y_r)
    _bcast_wait(me, yg, y_s, y_r)
    for c in range(N):
        y[:, c * C:(c + 1) * C] = yg[c]


def _k4(lens, y, k0, v0, k1, v1, kin, vin, kn, vn, yo, sem):
    me = lax.axis_index('sp')
    for wait in (False, True):
        for b in range(B):
            p = lens[b] - 1 - me * SD

            @pl.when((p >= 0) & (p < SD))
            def _():
                for i, (src, dst) in enumerate(((k0, kn.at[0]), (v0, vn.at[0]), (k1, kn.at[1]), (v1, vn.at[1]))):
                    c = pltpu.make_async_copy(src.at[b], dst.at[b, jnp.clip(p, 0, SD - 1)], sem.at[i, b])
                    c.wait() if wait else c.start()
        if not wait:
            yo[...] = y[...]


def solution(mesh):
    kspec = P(None, 'dp', 'sp', None, None)

    def local(x, lens, wq, wk, wv, wo, w1, w2, g1, g2, kc, vc):
        kc4, vc4 = (c.reshape(2, B, R, DH) for c in (kc, vc))
        qkv0 = pl.pallas_call(
            _k1, name='k1', out_shape=SDS((N, B, QW), BF16), in_specs=[VM, VM, HBM, HBM, HBM], out_specs=VM,
            scratch_shapes=[pltpu.VMEM((B, D), BF16), pltpu.VMEM((D, G * DH), BF16), pltpu.VMEM((2, D, DH), BF16),
                            DMA((3,)), DMA((N,)), DMA((N,))],
            compiler_params=pltpu.CompilerParams(collective_id=0, has_side_effects=True, vmem_limit_bytes=LIMIT),
        )(x, g1, wq, wk, wv)
        new = SDS((B, KVH, DH), BF16)
        kn, vn, o0, ml0, k0, v0 = pl.pallas_call(
            _k2, name='k2',
            out_shape=(pltpu.HBM(kc4.shape, BF16), pltpu.HBM(vc4.shape, BF16), SDS((N * G * B, DH), F32),
                       SDS((N * B, DH), F32), new, new),
            in_specs=[SM, VM, HBM, HBM], out_specs=(HBM, HBM, VM, VM, VM, VM),
            scratch_shapes=[pltpu.VMEM((G + 2, N * B, DH), F32), pltpu.VMEM((2, B, R, DH), BF16),
                            pltpu.VMEM((2, B, R, DH), BF16), DMA((2, 2, B)), DMA((2, 2, B))],
            compiler_params=pltpu.CompilerParams(vmem_limit_bytes=LIMIT),
        )(lens, qkv0, kc4, vc4)
        y, k1, v1 = pl.pallas_call(
            _main, name='main', out_shape=(SDS((B, D), BF16), new, new),
            in_specs=[VM, SM, VM, VM, VM, VM, VM] + [HBM] * 8, out_specs=(VM, VM, VM),
            scratch_shapes=[
                pltpu.VMEM((D, G * DH), BF16), pltpu.VMEM((2, D, DH), BF16), pltpu.VMEM((N, G * DH, C), BF16),
                pltpu.VMEM((NF, D, FC), BF16), pltpu.VMEM((N, FD, C), BF16), pltpu.VMEM((B, R, DH), BF16),
                pltpu.VMEM((B, R, DH), BF16), pltpu.VMEM((B, D), BF16), pltpu.VMEM((B, FD), BF16),
                pltpu.VMEM((N, B, QW), BF16), pltpu.VMEM((G + 2, N * B, DH), F32), pltpu.VMEM((N * G * B, DH), F32),
                pltpu.VMEM((2, N, G * B, DH), F32), pltpu.VMEM((2, N, B, DH), F32), pltpu.VMEM((4, N, B, C), F32),
                pltpu.VMEM((4, N, B, C), F32), pltpu.VMEM((3, N, B, C), F32), pltpu.VMEM((N, B, C), BF16),
                pltpu.VMEM((N * B, DH), F32),
                DMA((3,)), DMA((N,)), DMA((NF,)), DMA((N,)), DMA((B,)), DMA((B,)),
                DMA((2, N)), DMA((2, N)), DMA((2, N)), DMA((2, N)), DMA((4, N)), DMA((4, N)), DMA((3, N)), DMA((3, N)),
                DMA((N,)), DMA((N,)), DMA((N,)), DMA((N,))],
            compiler_params=pltpu.CompilerParams(collective_id=1, has_side_effects=True, vmem_limit_bytes=LIMIT),
        )(x, lens, g1, g2, qkv0, o0, ml0, wq, wk, wv, wo, w1, w2, kc4, vc4)
        shape = kc.shape
        kn, vn, y = pl.pallas_call(
            _k4, name='k4', out_shape=(pltpu.HBM(shape, BF16), pltpu.HBM(shape, BF16), SDS((B, D), BF16)),
            in_specs=[SM, VM, VM, VM, VM, VM, HBM, HBM], out_specs=(HBM, HBM, VM), input_output_aliases={6: 0, 7: 1},
            scratch_shapes=[DMA((4, B))],
            compiler_params=pltpu.CompilerParams(vmem_limit_bytes=LIMIT),
        )(lens, y, k0, v0, k1, v1, kn.reshape(shape), vn.reshape(shape))
        return y, kn, vn

    return jax.shard_map(
        local, mesh=mesh,
        in_specs=(P('dp', None), P('dp'), P(), P(), P(), P(None, 'sp', None), P(None, None, 'sp'),
                  P(None, 'sp', None), P(), P(), kspec, kspec),
        out_specs=(P('dp', None), kspec, kspec), check_vma=False)
```
